16 devices in a mesh: tp: 16 (over z, y, x, core).
Axes of the slice: x: 2, y: 2, z: 2, core: 2. Of those that a mesh axis runs over, the one named last changes fastest.
Arguments:
- hidden_in: bfloat16 [2, 3072, 3584], P(None, 'tp')
- lengths: int32 [2], replicated
- attn_norm: bfloat16 [2, 3584], replicated
- w_query: bfloat16 [2, 3584, 28, 128], replicated
- w_key: bfloat16 [2, 3584, 4, 128], replicated
- w_value: bfloat16 [2, 3584, 4, 128], replicated
- w_out: bfloat16 [2, 28, 128, 3584], replicated
- mlp_norm: bfloat16 [2, 3584], replicated
- w_gate: bfloat16 [2, 3584, 18944], P(None, None, 'tp')
- w_up: bfloat16 [2, 3584, 18944], P(None, None, 'tp')
- w_down: bfloat16 [2, 18944, 3584], P(None, 'tp')
- final_norm: bfloat16 [3584], replicated
Outputs:
- output: bfloat16 [2, 3072, 3584], P(None, 'tp')
All inputs are finite; a program needn't handle non-finite values.
Results may differ from the reference program's by a relative error of at most 0.02.
Values are sent between devices in bfloat16 or wider.
A program may use at most 1 GiB of HBM per device.

```python
import jax
import jax.numpy as jnp
from jax import lax

BATCH = 2
SEQ_DEV = 192
TP_SIZE = 16
SEQ_LEN = 3072
D_MODEL = 3584
HEADS = 28
KV_HEADS = 4
HEAD_DIM = 128
FF_DIM = 18944
LAYERS = 2

NORM_EPS = 1e-5
ROPE_BASE = 500000.0


def setup_inputs(seed: int = 0) -> dict:
    keys = jax.random.split(jax.random.key(seed), 12)
    d_scale = D_MODEL ** -0.5
    hidden_in = jax.random.normal(keys[0], (BATCH, SEQ_LEN, D_MODEL), jnp.float32)
    lengths = jax.random.randint(keys[1], (BATCH,), 1, SEQ_LEN + 1, jnp.int32)
    attn_norm = 1.0 + 0.25 * jax.random.normal(keys[2], (LAYERS, D_MODEL), jnp.float32)
    w_query = 1.4 * d_scale * jax.random.normal(keys[3], (LAYERS, D_MODEL, HEADS, HEAD_DIM), jnp.float32)
    w_key = 1.4 * d_scale * jax.random.normal(keys[4], (LAYERS, D_MODEL, KV_HEADS, HEAD_DIM), jnp.float32)
    w_value = d_scale * jax.random.normal(keys[5], (LAYERS, D_MODEL, KV_HEADS, HEAD_DIM), jnp.float32)
    w_out = (HEADS * HEAD_DIM) ** -0.5 * jax.random.normal(keys[6], (LAYERS, HEADS, HEAD_DIM, D_MODEL), jnp.float32)
    mlp_norm = 1.0 + 0.25 * jax.random.normal(keys[7], (LAYERS, D_MODEL), jnp.float32)
    w_gate = d_scale * jax.random.normal(keys[8], (LAYERS, D_MODEL, FF_DIM), jnp.float32)
    w_up = d_scale * jax.random.normal(keys[9], (LAYERS, D_MODEL, FF_DIM), jnp.float32)
    w_down = FF_DIM ** -0.5 * jax.random.normal(keys[10], (LAYERS, FF_DIM, D_MODEL), jnp.float32)
    final_norm = 1.0 + 0.25 * jax.random.normal(keys[11], (D_MODEL,), jnp.float32)
    return {
        'hidden_in': hidden_in.astype(jnp.bfloat16),
        'lengths': lengths,
        'attn_norm': attn_norm.astype(jnp.bfloat16),
        'w_query': w_query.astype(jnp.bfloat16),
        'w_key': w_key.astype(jnp.bfloat16),
        'w_value': w_value.astype(jnp.bfloat16),
        'w_out': w_out.astype(jnp.bfloat16),
        'mlp_norm': mlp_norm.astype(jnp.bfloat16),
        'w_gate': w_gate.astype(jnp.bfloat16),
        'w_up': w_up.astype(jnp.bfloat16),
        'w_down': w_down.astype(jnp.bfloat16),
        'final_norm': final_norm.astype(jnp.bfloat16),
    }


def rms_norm(hidden, gain):
    h_wide = hidden.astype(jnp.float32)
    inv_rms = lax.rsqrt(jnp.mean(h_wide * h_wide, axis=-1, keepdims=True) + NORM_EPS)
    return (h_wide * inv_rms * gain.astype(jnp.float32)).astype(jnp.bfloat16)


def rotate(proj, cos_tab, sin_tab):
    half_dim = proj.shape[-1] // 2
    first = proj[..., :half_dim]
    second = proj[..., half_dim:]
    return jnp.concatenate([first * cos_tab - second * sin_tab, second * cos_tab + first * sin_tab], axis=-1)


def reference(hidden_in, lengths, attn_norm, w_query, w_key, w_value, w_out, mlp_norm, w_gate, w_up, w_down, final_norm):
    groups = HEADS // KV_HEADS
    ff_shard = FF_DIM // TP_SIZE
    half_dim = HEAD_DIM // 2
    positions = jnp.arange(SEQ_LEN)
    inv_freq = ROPE_BASE ** (-2.0 * jnp.arange(half_dim).astype(jnp.float32) / HEAD_DIM)
    angles = positions.astype(jnp.float32)[:, None, None] * inv_freq[None, None, :]
    cos_tab = jnp.cos(angles)
    sin_tab = jnp.sin(angles)
    score_scale = HEAD_DIM ** -0.5
    key_ok = positions[None, :] < lengths[:, None]

    def layer_fn(hidden, layer_w):
        g_attn, w_q, w_k, w_v, w_o, g_mlp, w_g, w_u, w_d = layer_w
        normed = rms_norm(hidden, g_attn).astype(jnp.float32)
        q_proj = jnp.einsum('bsd,dhe->bshe', normed, w_q.astype(jnp.float32))
        key_proj = jnp.einsum('bsd,dhe->bshe', normed, w_k.astype(jnp.float32))
        v_proj = jnp.einsum('bsd,dhe->bshe', normed, w_v.astype(jnp.float32)).astype(jnp.bfloat16)
        q_rot = rotate(q_proj, cos_tab, sin_tab).astype(jnp.bfloat16)
        k_rot = rotate(key_proj, cos_tab, sin_tab).astype(jnp.bfloat16)
        q_blocks = jnp.moveaxis(q_rot.reshape(BATCH, TP_SIZE, SEQ_DEV, KV_HEADS, groups, HEAD_DIM), 1, 0)
        k_wide = k_rot.astype(jnp.float32)
        v_wide = v_proj.astype(jnp.float32)

        def block_fn(blk_args):
            q_blk, blk_idx = blk_args
            q_pos = blk_idx * SEQ_DEV + jnp.arange(SEQ_DEV)
            scores = jnp.einsum('bqkgd,bskd->bkgqs', q_blk.astype(jnp.float32), k_wide) * score_scale
            allowed = (positions[None, None, :] <= q_pos[None, :, None]) & key_ok[:, None, :]
            scores = jnp.where(allowed[:, None, None, :, :], scores, -1e30)
            prob_mat = jax.nn.softmax(scores, axis=-1).astype(jnp.bfloat16)
            context = jnp.einsum('bkgqs,bskd->bqkgd', prob_mat.astype(jnp.float32), v_wide)
            return context.astype(jnp.bfloat16)

        context = lax.map(block_fn, (q_blocks, jnp.arange(TP_SIZE)))
        context = jnp.moveaxis(context, 0, 1).reshape(BATCH, SEQ_LEN, HEADS, HEAD_DIM)
        attn_out = jnp.einsum('bshe,hed->bsd', context.astype(jnp.float32), w_o.astype(jnp.float32))
        hidden = (hidden.astype(jnp.float32) + attn_out).astype(jnp.bfloat16)
        normed = rms_norm(hidden, g_mlp).reshape(BATCH * SEQ_LEN, D_MODEL)
        wg_shards = jnp.moveaxis(w_g.reshape(D_MODEL, TP_SIZE, ff_shard), 1, 0)
        wu_shards = jnp.moveaxis(w_u.reshape(D_MODEL, TP_SIZE, ff_shard), 1, 0)
        wd_shards = w_d.reshape(TP_SIZE, ff_shard, D_MODEL)

        def shard_fn(acc_sum, shard_w):
            g_w, u_w, d_w = shard_w
            gate_proj = jnp.dot(normed, g_w, preferred_element_type=jnp.float32)
            up_proj = jnp.dot(normed, u_w, preferred_element_type=jnp.float32)
            gated_act = (jax.nn.silu(gate_proj) * up_proj).astype(jnp.bfloat16)
            part_out = jnp.dot(gated_act, d_w, preferred_element_type=jnp.float32).astype(jnp.bfloat16)
            return acc_sum + part_out.astype(jnp.float32), None

        mlp_out, unused = lax.scan(shard_fn, jnp.zeros((BATCH * SEQ_LEN, D_MODEL), jnp.float32), (wg_shards, wu_shards, wd_shards))
        hidden = (hidden.astype(jnp.float32) + mlp_out.reshape(BATCH, SEQ_LEN, D_MODEL)).astype(jnp.bfloat16)
        return hidden, None

    hidden, unused = lax.scan(layer_fn, hidden_in, (attn_norm, w_query, w_key, w_value, w_out, mlp_norm, w_gate, w_up, w_down))
    return rms_norm(hidden, final_norm)
```

```python
import jax
import jax.numpy as jnp
from jax import lax
from jax.sharding import PartitionSpec as P

NORM_EPS = 1e-5
ROPE_BASE = 500000.0


def rms_norm(hidden, gain):
    h_wide = hidden.astype(jnp.float32)
    inv_rms = lax.rsqrt(jnp.mean(h_wide * h_wide, axis=-1, keepdims=True) + NORM_EPS)
    return (h_wide * inv_rms * gain.astype(jnp.float32)).astype(jnp.bfloat16)


def rope_tables(positions, head_dim):
    half_dim = head_dim // 2
    inv_freq = ROPE_BASE ** (-2.0 * jnp.arange(half_dim).astype(jnp.float32) / head_dim)
    angles = positions.astype(jnp.float32)[:, None, None] * inv_freq[None, None, :]
    return jnp.cos(angles), jnp.sin(angles)


def rotate(proj, cos_tab, sin_tab):
    half_dim = proj.shape[-1] // 2
    first = proj[..., :half_dim]
    second = proj[..., half_dim:]
    return jnp.concatenate([first * cos_tab - second * sin_tab, second * cos_tab + first * sin_tab], axis=-1)


def attend(q_rot, k_all, v_all, q_pos, lengths):
    head_dim = q_rot.shape[-1]
    key_pos = jnp.arange(k_all.shape[1])
    allowed = (key_pos[None, None, :] <= q_pos[None, :, None]) & (key_pos[None, None, :] < lengths[:, None, None])
    scores = jnp.einsum('bqkgd,bskd->bkgqs', q_rot, k_all, preferred_element_type=jnp.float32) * (head_dim ** -0.5)
    scores = jnp.where(allowed[:, None, None, :, :], scores, -1e30)
    prob_mat = jax.nn.softmax(scores, axis=-1).astype(jnp.bfloat16)
    context = jnp.einsum('bkgqs,bskd->bqkgd', prob_mat, v_all, preferred_element_type=jnp.float32)
    return context.astype(jnp.bfloat16)


def solution(mesh):
    tp_size = mesh.shape['tp']

    def device_fn(hidden_in, lengths, attn_norm, w_query, w_key, w_value, w_out, mlp_norm, w_gate, w_up, w_down, final_norm):
        batch, seq_dev, d_model = hidden_in.shape
        heads = w_query.shape[2]
        head_dim = w_query.shape[3]
        kv_heads = w_key.shape[2]
        groups = heads // kv_heads
        q_pos = lax.axis_index('tp') * seq_dev + jnp.arange(seq_dev)
        cos_tab, sin_tab = rope_tables(q_pos, head_dim)
        hidden = hidden_in
        for layer in range(w_query.shape[0]):
            normed = rms_norm(hidden, attn_norm[layer])
            q_proj = jnp.einsum('bsd,dhe->bshe', normed, w_query[layer], preferred_element_type=jnp.float32)
            k_proj = jnp.einsum('bsd,dhe->bshe', normed, w_key[layer], preferred_element_type=jnp.float32)
            v_proj = jnp.einsum('bsd,dhe->bshe', normed, w_value[layer], preferred_element_type=jnp.float32).astype(jnp.bfloat16)
            q_rot = rotate(q_proj, cos_tab, sin_tab).astype(jnp.bfloat16).reshape(batch, seq_dev, kv_heads, groups, head_dim)
            k_rot = rotate(k_proj, cos_tab, sin_tab).astype(jnp.bfloat16)
            k_all = lax.all_gather(k_rot, 'tp', axis=1, tiled=True)
            v_all = lax.all_gather(v_proj, 'tp', axis=1, tiled=True)
            context = attend(q_rot, k_all, v_all, q_pos, lengths).reshape(batch, seq_dev, heads, head_dim)
            attn_out = jnp.einsum('bshe,hed->bsd', context, w_out[layer], preferred_element_type=jnp.float32)
            hidden = (hidden.astype(jnp.float32) + attn_out).astype(jnp.bfloat16)
            normed = rms_norm(hidden, mlp_norm[layer])
            full_normed = lax.all_gather(normed, 'tp', axis=1, tiled=True)
            gate_proj = jnp.einsum('bsd,df->bsf', full_normed, w_gate[layer], preferred_element_type=jnp.float32)
            up_proj = jnp.einsum('bsd,df->bsf', full_normed, w_up[layer], preferred_element_type=jnp.float32)
            gated_act = (jax.nn.silu(gate_proj) * up_proj).astype(jnp.bfloat16)
            part_out = jnp.einsum('bsf,fd->bsd', gated_act, w_down[layer], preferred_element_type=jnp.float32)
            part_out = lax.reduce_precision(part_out, 8, 7)
            mlp_out = lax.psum_scatter(part_out, 'tp', scatter_dimension=1, tiled=True)
            hidden = (hidden.astype(jnp.float32) + mlp_out).astype(jnp.bfloat16)
        return rms_norm(hidden, final_norm)

    seq_part = P(None, 'tp', None)
    in_specs = (seq_part, P(), P(), P(), P(), P(), P(), P(), P(None, None, 'tp'), P(None, None, 'tp'), P(None, 'tp', None), P())
    return jax.shard_map(device_fn, mesh=mesh, in_specs=in_specs, out_specs=seq_part, check_vma=False)
```

```python
import jax
import jax.numpy as jnp
from jax import lax
from jax.sharding import PartitionSpec as P

NORM_EPS = 1e-5
ROPE_BASE = 500000.0
AXIS_BIT = {'z': 8, 'y': 4, 'x': 2, 'core': 1}
COLOURS = (('x', 'y', 'z'), ('y', 'z', 'x'), ('z', 'x', 'y'))


def rms_norm(hidden, gain):
    h_wide = hidden.astype(jnp.float32)
    inv_rms = lax.rsqrt(jnp.mean(h_wide * h_wide, axis=-1, keepdims=True) + NORM_EPS)
    return (h_wide * inv_rms * gain.astype(jnp.float32)).astype(jnp.bfloat16)


def rope_tables(positions, head_dim):
    half_dim = head_dim // 2
    inv_freq = ROPE_BASE ** (-2.0 * jnp.arange(half_dim).astype(jnp.float32) / head_dim)
    angles = positions.astype(jnp.float32)[:, None, None] * inv_freq[None, None, :]
    return jnp.cos(angles), jnp.sin(angles)


def rotate(proj, cos_tab, sin_tab):
    half_dim = proj.shape[-1] // 2
    first = proj[..., :half_dim]
    second = proj[..., half_dim:]
    return jnp.concatenate([first * cos_tab - second * sin_tab, second * cos_tab + first * sin_tab], axis=-1)


def attend(q_rot, k_all, v_all, q_pos, length):
    head_dim = q_rot.shape[-1]
    key_pos = jnp.arange(k_all.shape[0])
    allowed = (key_pos[None, :] <= q_pos[:, None]) & (key_pos[None, :] < length)
    scores = jnp.einsum('qkgd,skd->kgqs', q_rot, k_all, preferred_element_type=jnp.float32) * (head_dim ** -0.5)
    scores = jnp.where(allowed[None, None, :, :], scores, -1e30)
    prob_mat = jax.nn.softmax(scores, axis=-1).astype(jnp.bfloat16)
    context = jnp.einsum('kgqs,skd->qkgd', prob_mat, v_all, preferred_element_type=jnp.float32)
    return context.astype(jnp.bfloat16)


def solution(mesh):
    tp_size = mesh.shape['tp']

    def swap(arr, axis):
        bit = AXIS_BIT[axis]
        return lax.ppermute(arr, 'tp', [(i, i ^ bit) for i in range(tp_size)])

    def device_fn(hidden_in, lengths, attn_norm, w_query, w_key, w_value, w_out, mlp_norm, w_gate, w_up, w_down, final_norm):
        batch, seq_dev, d_model = hidden_in.shape
        heads = w_query.shape[2]
        head_dim = w_query.shape[3]
        kv_heads = w_key.shape[2]
        groups = heads // kv_heads
        me = lax.axis_index('tp')
        mine = {name: (me // bit) % 2 for name, bit in AXIS_BIT.items()}
        q_pos = me * seq_dev + jnp.arange(seq_dev)
        cos_tab, sin_tab = rope_tables(q_pos, head_dim)

        def pick(arr, names, axis, side):
            dim = names.index(axis)
            return lax.dynamic_index_in_dim(arr, side, dim, keepdims=False), [n for n in names if n != axis]

        def reduce_scatter(part):
            part = part.reshape(2, 2, 2, 2, seq_dev, d_model)
            names = ['z', 'y', 'x', 'core']
            away, rest = pick(part, names, 'core', 1 - mine['core'])
            own, rest = pick(part, names, 'core', mine['core'])
            got = swap(away, 'core')
            third = seq_dev // 3
            sums = []
            for c in range(3):
                rows = slice(c * third, (c + 1) * third)
                sums.append(own[..., rows, :].astype(jnp.float32) + got[..., rows, :].astype(jnp.float32))
            left = [list(rest) for _ in range(3)]
            for phase in range(3):
                sent = []
                for c in range(3):
                    axis = COLOURS[c][phase]
                    send, _ = pick(sums[c], left[c], axis, 1 - mine[axis])
                    sent.append(swap(send, axis))
                for c in range(3):
                    axis = COLOURS[c][phase]
                    keep, left[c] = pick(sums[c], left[c], axis, mine[axis])
                    sums[c] = keep + sent[c]
            return jnp.concatenate(sums, axis=0)

        hidden = [hidden_in[b] for b in range(batch)]
        for layer in range(w_query.shape[0]):
            q_rots, kv_alls, zs, parts = [], [], [], []
            for b in range(batch):
                normed = rms_norm(hidden[b], attn_norm[layer])
                k_proj = jnp.einsum('sd,dhe->she', normed, w_key[layer], preferred_element_type=jnp.float32)
                v_proj = jnp.einsum('sd,dhe->she', normed, w_value[layer], preferred_element_type=jnp.float32).astype(jnp.bfloat16)
                k_rot = rotate(k_proj, cos_tab, sin_tab).astype(jnp.bfloat16)
                kv_alls.append(lax.all_gather(jnp.concatenate([k_rot, v_proj], axis=1), 'tp', axis=0, tiled=True))
                q_proj = jnp.einsum('sd,dhe->she', normed, w_query[layer], preferred_element_type=jnp.float32)
                q_rots.append(rotate(q_proj, cos_tab, sin_tab).astype(jnp.bfloat16).reshape(seq_dev, kv_heads, groups, head_dim))
            for b in range(batch):
                k_all, v_all = kv_alls[b][:, :kv_heads], kv_alls[b][:, kv_heads:]
                context = attend(q_rots[b], k_all, v_all, q_pos, lengths[b]).reshape(seq_dev, heads, head_dim)
                attn_out = jnp.einsum('she,hed->sd', context, w_out[layer], preferred_element_type=jnp.float32)
                hidden[b] = (hidden[b].astype(jnp.float32) + attn_out).astype(jnp.bfloat16)
                normed = rms_norm(hidden[b], mlp_norm[layer])
                zs.append(lax.all_gather(normed, 'tp', axis=0, tiled=True))
            for b in range(batch):
                gate_proj = jnp.einsum('sd,df->sf', zs[b], w_gate[layer], preferred_element_type=jnp.float32)
                up_proj = jnp.einsum('sd,df->sf', zs[b], w_up[layer], preferred_element_type=jnp.float32)
                gated_act = (jax.nn.silu(gate_proj) * up_proj).astype(jnp.bfloat16)
                parts.append(jnp.einsum('sf,fd->sd', gated_act, w_down[layer], preferred_element_type=jnp.float32).astype(jnp.bfloat16))
            for b in range(batch):
                mlp_out = reduce_scatter(parts[b])
                hidden[b] = (hidden[b].astype(jnp.float32) + mlp_out).astype(jnp.bfloat16)
        return jnp.stack([rms_norm(hidden[b], final_norm) for b in range(batch)])

    seq_part = P(None, 'tp', None)
    in_specs = (seq_part, P(), P(), P(), P(), P(), P(), P(), P(None, None, 'tp'), P(None, None, 'tp'), P(None, 'tp', None), P())
    return jax.shard_map(device_fn, mesh=mesh, in_specs=in_specs, out_specs=seq_part, check_vma=False)
```
